32 devices in a mesh: dp: 8 (over z, x), expert: 4 (over y, core).
Axes of the slice: x: 2, y: 2, z: 4, core: 2. Of those that a mesh axis runs over, the one named last changes fastest.
Arguments:
- tokens: bfloat16 [4096, 4096], P(('dp', 'expert')), may hold values from -6 to 6
- select: int32 [4, 128], P(None, ('dp', 'expert')), may hold values from -1 to 127, as said below
- gates: float32 [4, 128], P(None, ('dp', 'expert')), may hold values from 0.1 to 1
- w_gate: bfloat16 [4, 4096, 8192], P('expert', None, 'dp'), may hold values from -0.09375 to 0.09375
- w_up: bfloat16 [4, 4096, 8192], P('expert', None, 'dp'), may hold values from -0.09375 to 0.09375
- w_down: bfloat16 [4, 8192, 4096], P('expert', 'dp'), may hold values from -0.0625 to 0.0625
Outputs:
- mixed: bfloat16 [4096, 4096], P(('dp', 'expert'))
The draws below stay inside these ranges and needn't reach their ends.
Inputs may be any that keep to these rules, and one draw needn't show every extreme that they name: `select`: in each block of 4 slots of a row, the live entries come first, distinct and ascending, below 128, followed by -1; every block holds at least one live entry, and every expert fills all 4 slots of some source device.
All inputs are finite; a program needn't handle non-finite values.
Results may differ from the reference program's by a relative error of at most 0.0085.
Values may be sent and summed in bfloat16 or wider, within the bound.
A program may use at most 64 MiB of HBM per device.

```python
import jax
import jax.numpy as jnp

D = 4096
FF = 8192
TOK_DEV = 128
EXPERTS = 4
SLOT = 4
TOKENS = 4096
DEVICES = 32


def draw_select(key, part):
    keys_all = jax.random.split(jax.random.fold_in(key, 11), EXPERTS * DEVICES)

    def one_block(sub_key):
        chosen = jax.random.permutation(sub_key, TOK_DEV)[:SLOT]
        return jnp.sort(chosen)
    picks = jax.vmap(one_block)(keys_all).reshape(EXPERTS, DEVICES, SLOT)
    counts = jax.random.randint(jax.random.fold_in(key, 7), (EXPERTS, DEVICES), 1, SLOT + 1)
    full_src = (jnp.arange(EXPERTS)[:, None] * 37 + 3) % DEVICES
    counts = jnp.where(jnp.arange(DEVICES)[None, :] == full_src, SLOT, counts)
    slot_pos = jnp.arange(SLOT)
    result = jnp.where(slot_pos[None, None, :] < counts[:, :, None], picks, -1)
    return result.reshape(EXPERTS, DEVICES * SLOT).astype(jnp.int32)


def steps_of(key, dims, cuts, least, top_value):
    def one(axis_at, shards_of):
        draws = jax.random.uniform(jax.random.fold_in(jax.random.fold_in(key, 6), axis_at), (shards_of,), jnp.float32, least / len(cuts), top_value / len(cuts))
        return jnp.repeat(jnp.exp(draws), dims[axis_at] // shards_of).reshape((-1,) + (1,) * (len(dims) - axis_at - 1))

    level = one(*cuts[0])
    for cut in cuts[1:]:
        level = level * one(*cut)
    return level


def bell_draw(own_key, extent, scale, bound, pieces=(), held_as=jnp.bfloat16):
    values = jax.random.normal(own_key, extent, jnp.float32) * scale
    if len(pieces) > 0:
        values = steps_of(own_key, extent, pieces, -0.22, 0.18) * values
    return jnp.clip(values, min=-bound, max=bound).astype(held_as)


def setup_inputs(seed: int = 0) -> dict:
    key_of = jax.random.split(jax.random.key(seed), 7)
    tokens = bell_draw(key_of[0], (TOKENS, D), 1.0, 6.0, ((0, 32),))
    select = draw_select(jax.random.fold_in(key_of[6], 71), 0)
    gates = jnp.clip(0.1 + 0.9 * jax.random.uniform(key_of[2], (EXPERTS, DEVICES * SLOT), jnp.float32) ** steps_of(key_of[2], (EXPERTS, DEVICES * SLOT), ((1, 32),), -0.2, 0.2), 0.1, 1.0)
    w_gate = bell_draw(key_of[3], (EXPERTS, D, FF), D ** -0.5, 0.09375, ((0, 4), (2, 8)))
    w_up = bell_draw(key_of[4], (EXPERTS, D, FF), D ** -0.5, 0.09375, ((0, 4), (2, 8)))
    w_down = bell_draw(key_of[5], (EXPERTS, FF, D), FF ** -0.5, 0.0625, ((0, 4), (1, 8)))
    return {"tokens": tokens, "select": select, "gates": gates, "w_gate": w_gate, "w_up": w_up, "w_down": w_down}


def reference(tokens, select, gates, w_gate, w_up, w_down):
    mixed = jnp.zeros((TOKENS, D), jnp.float32)
    source = (jnp.arange(DEVICES * SLOT) // SLOT).astype(jnp.int32)
    for expert_id in range(EXPERTS):
        index_row = select[expert_id]
        is_live = index_row >= 0
        global_idx = (source * TOK_DEV + jnp.where(is_live, index_row, 0)).astype(jnp.int32)
        sel_rows = jnp.where(is_live[:, None], tokens[global_idx], 0).astype(jnp.bfloat16)
        gate_val = jnp.dot(sel_rows, w_gate[expert_id], preferred_element_type=jnp.float32)
        up_val = jnp.dot(sel_rows, w_up[expert_id], preferred_element_type=jnp.float32)
        hidden = (jax.nn.silu(gate_val) * up_val).astype(jnp.bfloat16)
        expert_out = jnp.dot(hidden, w_down[expert_id], preferred_element_type=jnp.float32).astype(jnp.bfloat16)
        weight_col = jnp.where(is_live, gates[expert_id], 0.0).astype(jnp.float32)
        mixed = mixed.at[global_idx].add(weight_col[:, None] * expert_out.astype(jnp.float32))
    return mixed.astype(jnp.bfloat16)
```

```python
import functools

import jax
import jax.numpy as jnp
from jax import lax
from jax.experimental import pallas as pl
from jax.experimental.pallas import tpu as pltpu
from jax.sharding import PartitionSpec as P

MESH = pl.DeviceIdType.MESH
TILE = 16
F32 = jnp.float32
BF16 = jnp.bfloat16


def log2(n):
    return n.bit_length() - 1


def kernel(
    nd, ne, tok_hbm, sel, gat, wg_hbm, wu_hbm, wd_hbm, ob, cmb,
    tok, wg, wu, wd, sb, ab, x, g_acc, u_acc, hid, pb, xr, zb, zr, summed, rb,
    t_sem, w_sem, a_send, a_recv, gz_send, gz_recv, gx_send, gx_recv,
    rx_send, rx_recv, rz_send, rz_recv, o_send, o_recv,
):
    stages = x.shape[0]
    inner = x.shape[1]
    outer = x.shape[2]
    rows = x.shape[3]
    span = x.shape[4]
    slots = sel.shape[1]
    tokens_here = tok.shape[0]
    parts = TILE // slots
    wide = span // parts
    chunks = pb.shape[0]
    cols = pb.shape[4]
    dp = lax.axis_index("dp")
    ex = lax.axis_index("expert")
    za = dp // inner
    xb = lax.rem(dp, inner)
    other = (inner - 1) - xb

    def at_expert(d):
        return (dp, lax.rem(ex + d, ne))

    def at_outer(d):
        return (lax.rem(za + d, outer) * inner + xb, ex)

    partner = (za * inner + other, ex)

    def remote(src, dst, send, recv, to):
        return pltpu.make_async_remote_copy(
            src_ref=src, dst_ref=dst, send_sem=send, recv_sem=recv,
            device_id=to, device_id_type=MESH,
        )

    barrier = pltpu.get_barrier_semaphore()
    for d in range(1, ne):
        pl.semaphore_signal(barrier, inc=1, device_id=at_expert(d), device_id_type=MESH)
    for d in range(1, outer):
        pl.semaphore_signal(barrier, inc=1, device_id=at_outer(d), device_id_type=MESH)
    if inner > 1:
        pl.semaphore_signal(barrier, inc=1, device_id=partner, device_id_type=MESH)

    fetch = pltpu.make_async_copy(tok_hbm, tok, t_sem)
    fetch.start()
    loads = [
        pltpu.make_async_copy(h.at[0], v, w_sem.at[i])
        for i, (h, v) in enumerate(((wg_hbm, wg), (wu_hbm, wu), (wd_hbm, wd)))
    ]
    for load in loads:
        load.start()

    packed = ne * TILE
    r_id = lax.broadcasted_iota(jnp.int32, (packed, tokens_here), 0)
    t_id = lax.broadcasted_iota(jnp.int32, (packed, tokens_here), 1)
    r_slot = ((r_id >> log2(TILE)) << log2(slots)) + (r_id & (slots - 1))
    r_part = (r_id & (TILE - 1)) >> log2(slots)
    named = jnp.full((packed, tokens_here), -1, jnp.int32)
    for e in range(ne):
        for s in range(slots):
            named = jnp.where(r_slot == e * slots + s, sel[e, s], named)
    hit = jnp.where(named == t_id, 1.0, 0.0)
    pick = jnp.concatenate(
        [jnp.where(r_part == p, hit, 0.0).astype(BF16) for p in range(parts)], axis=1
    )
    fetch.wait()
    for q in range(stages):
        stack = jnp.concatenate(
            [tok[:, q * span + p * wide:q * span + (p + 1) * wide] for p in range(parts)], axis=0
        )
        gathered = jnp.dot(pick, stack, preferred_element_type=F32).astype(BF16)
        sb[q] = gathered.reshape(ne, TILE, wide)
        ab[q, ex] = sb[q, ex]

    pl.semaphore_wait(barrier, (ne - 1) + (outer - 1) + (1 if inner > 1 else 0))

    sent = []

    def start(copy):
        copy.start()
        sent.append(copy)

    for q in range(stages):
        for d in range(1, ne):
            to = at_expert(d)
            start(remote(sb.at[q, to[1]], ab.at[q, ex], a_send.at[q, d], a_recv.at[q, d], to))

    def packing(shape, packed_dim):
        r = lax.broadcasted_iota(jnp.int32, shape, packed_dim)
        k = lax.broadcasted_iota(jnp.int32, shape, 1 - packed_dim)
        col = (
            ((r & (TILE - 1)) >> log2(slots)) * rows
            + ((r >> log2(TILE)) << log2(slots)) + (r & (slots - 1))
        )
        return jnp.where(k == col, 1.0, 0.0).astype(BF16)

    pack = packing((packed, parts * rows), 0)
    unpack = packing((parts * rows, packed), 1)

    def gx(q, owner_b, d):
        block = x.at[q, owner_b, lax.rem(za + outer - d, outer)]
        return remote(block, block, gx_send.at[q, d], gx_recv.at[q, d], partner)

    def gz(q, d, owner_a):
        block = x.at[q, xb, owner_a]
        return remote(block, block, gz_send.at[q, d], gz_recv.at[q, d], at_outer(d))

    order = sorted(range(1, outer), key=lambda d: (min(d, outer - d), d))
    for q in range(stages):
        for d in range(1, ne):
            src = lax.rem(ex + ne - d, ne)
            remote(
                sb.at[q, src], ab.at[q, src], a_send.at[q, d], a_recv.at[q, d], at_expert(d)
            ).wait_recv()
        mine = jnp.dot(
            unpack, ab[q].reshape(packed, wide), preferred_element_type=F32
        ).astype(BF16)
        for p in range(parts):
            x[q, xb, za, :, p * wide:(p + 1) * wide] = mine[p * rows:(p + 1) * rows]
        for d in order:
            start(gz(q, d, za))
        if inner > 1:
            start(gx(q, xb, 0))

    terms = 3
    c_id = lax.broadcasted_iota(jnp.int32, (tokens_here, terms * packed), 1)
    n_id = lax.broadcasted_iota(jnp.int32, (tokens_here, terms * packed), 0)
    c_row = c_id & (packed - 1)
    c_slot = ((c_row >> log2(TILE)) << log2(slots)) + (c_row & (slots - 1))
    weight = jnp.zeros((tokens_here, terms * packed), F32)
    for e in range(ne):
        for s in range(slots):
            weight = jnp.where((c_slot == e * slots + s) & (n_id == sel[e, s]), gat[e, s], weight)
    left = weight
    coef = jnp.zeros_like(weight)
    for i in range(terms):
        term = left.astype(BF16).astype(F32)
        coef = jnp.where((c_id >> log2(packed)) == i, term, coef)
        left = left - term
    c_part = (c_row & (TILE - 1)) >> log2(slots)
    for p in range(parts):
        cmb[p] = jnp.where(c_part == p, coef, 0.0).astype(BF16)

    total_rows = inner * outer * rows
    step = min(256, hid.shape[1])

    def arrive(q):
        for d in order:
            gz(q, d, lax.rem(za + outer - d, outer)).wait_recv()
            if inner > 1:
                start(gx(q, xb, d))

    def multiply(q):
        if inner > 1:
            for d in [0] + order:
                gx(q, other, d).wait_recv()
        if q == 0:
            loads[0].wait()
            loads[1].wait()

        @pl.loop(0, hid.shape[1] // step, unroll=True)
        def _(i):
            at = pl.ds(pl.multiple_of(i * step, step), step)
            block = x[q].reshape(total_rows, span)
            g = jnp.dot(block, wg[q * span:(q + 1) * span, at], preferred_element_type=F32)
            u = jnp.dot(block, wu[q * span:(q + 1) * span, at], preferred_element_type=F32)
            if q > 0:
                g = g + g_acc[:, at]
                u = u + u_acc[:, at]
            if q < stages - 1:
                g_acc[:, at] = g
                u_acc[:, at] = u
            else:
                hid[:, at] = (g / (1.0 + jnp.exp(-g)) * u).astype(BF16)

    for q in range(stages):
        arrive(q)
        if q > 0:
            multiply(q - 1)
    multiply(stages - 1)

    loads[2].wait()

    def rx(c):
        return remote(pb.at[c, other], xr.at[c], rx_send.at[c], rx_recv.at[c], partner)

    @pl.loop(0, chunks)
    def _(c):
        at = pl.ds(pl.multiple_of(c * cols, cols), cols)
        part = jnp.dot(hid[...], wd[:, at], preferred_element_type=F32)
        pb[c] = part.astype(BF16).reshape(inner, outer, rows, cols)
        if inner > 1:
            rx(c).start()

    def rz(c, d):
        to = lax.rem(za + d, outer)
        return remote(zb.at[c, to], zr.at[c, d - 1], rz_send.at[c, d], rz_recv.at[c, d], at_outer(d))

    def inner_sum(c):
        value = pb[c, xb].astype(F32)
        if inner > 1:
            rx(c).wait_recv()
            value = value + xr[c].astype(F32)
        zb[c] = value.astype(BF16)
        for d in order:
            rz(c, d).start()

    per = span // cols

    def outer_sum(c):
        value = zb[c, za].astype(F32)
        for d in order:
            rz(c, d).wait_recv()
            value = value + zr[c, d - 1].astype(F32)
        for k in range(cols // wide):
            p = (c % per) * (cols // wide) + k
            summed[c // per, p] = value[:, k * wide:(k + 1) * wide].astype(BF16)

    def give(q):
        back = jnp.dot(pack, summed[q].reshape(parts * rows, wide), preferred_element_type=F32)
        rb[q] = back.astype(BF16).reshape(ne, TILE, wide)
        ob[q, ex] = rb[q, ex]
        for d in range(1, ne):
            to = at_expert(d)
            start(remote(rb.at[q, to[1]], ob.at[q, ex], o_send.at[q, d], o_recv.at[q, d], to))

    lag = min(3, chunks)
    for c in range(chunks + lag):
        if c < chunks:
            inner_sum(c)
        done = c - lag
        if done >= 0:
            outer_sum(done)
            if done % per == per - 1:
                give(done // per)

    for q in range(stages):
        for d in range(1, ne):
            src = lax.rem(ex + ne - d, ne)
            remote(
                rb.at[q, src], ob.at[q, src], o_send.at[q, d], o_recv.at[q, d], at_expert(d)
            ).wait_recv()

    for copy in sent:
        copy.wait_send()

    @pl.loop(0, chunks)
    def _(c):
        if inner > 1:
            rx(c).wait_send()
        for d in range(1, outer):
            rz(c, d).wait_send()


def mix(ob, cmb, out_hbm, out, sem):
    stages, ne, tile, wide = ob.shape
    parts, tokens_here, depth = cmb.shape
    packed = ne * tile
    terms = depth // packed
    span = parts * wide
    stores = []
    for q in range(stages):
        got = ob[q].reshape(packed, wide)
        total = jnp.dot(
            cmb[...].reshape(parts * tokens_here, depth),
            jnp.concatenate([got] * terms, axis=0),
            preferred_element_type=F32,
        ).astype(BF16)
        for p in range(parts):
            at = q * span + p * wide
            out[:, at:at + wide] = total[p * tokens_here:(p + 1) * tokens_here]
        at = pl.ds(q * span, span)
        store = pltpu.make_async_copy(out.at[:, at], out_hbm.at[:, at], sem.at[q])
        store.start()
        stores.append(store)
    for store in stores:
        store.wait()


def per_device(nd, ne, tokens, select, gates, w_gate, w_up, w_down):
    tok_dev, width = tokens.shape
    slots = select.shape[1]
    hidden = w_gate.shape[2]
    inner = 2 if nd % 2 == 0 else 1
    outer = nd // inner
    rows = ne * slots
    parts = TILE // slots
    stages = 4
    span = width // stages
    wide = span // parts
    cols = span // 2
    chunks = width // cols
    vmem = pl.BlockSpec(memory_space=pltpu.VMEM)
    smem = pl.BlockSpec(memory_space=pltpu.SMEM)
    hbm = pl.BlockSpec(memory_space=pl.ANY)
    dma = pltpu.SemaphoreType.DMA
    returned, coef = pl.pallas_call(
        functools.partial(kernel, nd, ne),
        out_shape=(
            jax.ShapeDtypeStruct((stages, ne, TILE, wide), BF16),
            jax.ShapeDtypeStruct((parts, tok_dev, 3 * ne * TILE), BF16),
        ),
        in_specs=[hbm, smem, smem, hbm, hbm, hbm],
        out_specs=(vmem, vmem),
        scratch_shapes=[
            pltpu.VMEM((tok_dev, width), BF16),
            pltpu.VMEM((width, hidden), BF16),
            pltpu.VMEM((width, hidden), BF16),
            pltpu.VMEM((hidden, width), BF16),
            pltpu.VMEM((stages, ne, TILE, wide), BF16),
            pltpu.VMEM((stages, ne, TILE, wide), BF16),
            pltpu.VMEM((stages, inner, outer, rows, span), BF16),
            pltpu.VMEM((nd * rows, hidden), F32),
            pltpu.VMEM((nd * rows, hidden), F32),
            pltpu.VMEM((nd * rows, hidden), BF16),
            pltpu.VMEM((chunks, inner, outer, rows, cols), BF16),
            pltpu.VMEM((chunks, outer, rows, cols), BF16),
            pltpu.VMEM((chunks, outer, rows, cols), BF16),
            pltpu.VMEM((chunks, max(outer - 1, 1), rows, cols), BF16),
            pltpu.VMEM((stages, parts, rows, wide), BF16),
            pltpu.VMEM((stages, ne, TILE, wide), BF16),
            dma(()),
            dma((3,)),
            dma((stages, ne)), dma((stages, ne)),
            dma((stages, outer)), dma((stages, outer)),
            dma((stages, outer)), dma((stages, outer)),
            dma((chunks,)), dma((chunks,)),
            dma((chunks, outer)), dma((chunks, outer)),
            dma((stages, ne)), dma((stages, ne)),
        ],
        compiler_params=pltpu.CompilerParams(
            collective_id=0, has_side_effects=True, vmem_limit_bytes=60 * 1024 * 1024
        ),
    )(tokens, select, gates, w_gate, w_up, w_down)
    return pl.pallas_call(
        mix,
        out_shape=jax.ShapeDtypeStruct((tok_dev, width), BF16),
        in_specs=[vmem, vmem],
        out_specs=hbm,
        scratch_shapes=[pltpu.VMEM((tok_dev, width), BF16), dma((stages,))],
    )(returned, coef)


def solution(mesh):
    return jax.shard_map(
        functools.partial(per_device, mesh.shape["dp"], mesh.shape["expert"]),
        mesh=mesh,
        in_specs=(
            P(("dp", "expert"), None),
            P(None, ("dp", "expert")),
            P(None, ("dp", "expert")),
            P("expert", None, "dp"),
            P("expert", None, "dp"),
            P("expert", "dp", None),
        ),
        out_specs=P(("dp", "expert"), None),
        check_vma=False,
    )
```

```python
import functools

import jax
import jax.numpy as jnp
from jax import lax
from jax.experimental import pallas as pl
from jax.experimental.pallas import tpu as pltpu
from jax.sharding import PartitionSpec as P

MESH = pl.DeviceIdType.MESH
TILE = 16
F32 = jnp.float32
BF16 = jnp.bfloat16


def log2(n):
    return n.bit_length() - 1


def kernel(
    nd, ne, tok_hbm, sel_hbm, gat_hbm, wg_hbm, wu_hbm, wd_hbm, ob, cmb,
    tok, sel, gat, wg, wu, wd, sb, ab, x, g_acc, u_acc, hid, pb, xr, zb, zr, summed, rb,
    t_sem, s_sem, w_sem, a_send, a_recv, gz_send, gz_recv, gx_send, gx_recv,
    rx_send, rx_recv, rz_send, rz_recv, o_send, o_recv,
):
    stages = x.shape[0]
    inner = x.shape[1]
    outer = x.shape[2]
    rows = x.shape[3]
    span = x.shape[4]
    slots = sel.shape[1]
    tokens_here = tok.shape[0]
    parts = TILE // slots
    wide = span // parts
    chunks = pb.shape[0]
    cols = pb.shape[4]
    dp = lax.axis_index("dp")
    ex = lax.axis_index("expert")
    za = dp // inner
    xb = lax.rem(dp, inner)
    other = (inner - 1) - xb

    def at_expert(d):
        return (dp, lax.rem(ex + d, ne))

    def at_outer(d):
        return (lax.rem(za + d, outer) * inner + xb, ex)

    partner = (za * inner + other, ex)

    def remote(src, dst, send, recv, to):
        return pltpu.make_async_remote_copy(
            src_ref=src, dst_ref=dst, send_sem=send, recv_sem=recv,
            device_id=to, device_id_type=MESH,
        )

    fetch = pltpu.make_async_copy(tok_hbm, tok, t_sem)
    fetch.start()
    small = [
        pltpu.make_async_copy(h, v, s_sem.at[i])
        for i, (h, v) in enumerate(((sel_hbm, sel), (gat_hbm, gat)))
    ]
    for copy in small:
        copy.start()
    barrier = pltpu.get_barrier_semaphore()
    for d in range(1, ne):
        pl.semaphore_signal(barrier, inc=1, device_id=at_expert(d), device_id_type=MESH)
    for d in range(1, outer):
        pl.semaphore_signal(barrier, inc=1, device_id=at_outer(d), device_id_type=MESH)
    if inner > 1:
        pl.semaphore_signal(barrier, inc=1, device_id=partner, device_id_type=MESH)

    packed = ne * TILE
    small[0].wait()
    r_id = lax.broadcasted_iota(jnp.int32, (packed, tokens_here), 0)
    t_id = lax.broadcasted_iota(jnp.int32, (packed, tokens_here), 1)
    r_slot = ((r_id >> log2(TILE)) << log2(slots)) + (r_id & (slots - 1))
    r_part = (r_id & (TILE - 1)) >> log2(slots)
    named = jnp.full((packed, tokens_here), -1, jnp.int32)
    for e in range(ne):
        for s in range(slots):
            named = jnp.where(r_slot == e * slots + s, sel[e, s], named)
    hit = jnp.where(named == t_id, 1.0, 0.0)
    pick = jnp.concatenate(
        [jnp.where(r_part == p, hit, 0.0).astype(BF16) for p in range(parts)], axis=1
    )
    fetch.wait()
    loads = [
        pltpu.make_async_copy(h.at[0], v, w_sem.at[i])
        for i, (h, v) in enumerate(((wg_hbm, wg), (wu_hbm, wu), (wd_hbm, wd)))
    ]
    for load in loads:
        load.start()

    for q in range(stages):
        stack = jnp.concatenate(
            [tok[:, q * span + p * wide:q * span + (p + 1) * wide] for p in range(parts)], axis=0
        )
        gathered = jnp.dot(pick, stack, preferred_element_type=F32).astype(BF16)
        sb[q] = gathered.reshape(ne, TILE, wide)
        ab[q, ex] = sb[q, ex]

    pl.semaphore_wait(barrier, (ne - 1) + (outer - 1) + (1 if inner > 1 else 0))

    def start(copy):
        copy.start()

    for q in range(stages):
        for d in range(1, ne):
            to = at_expert(d)
            start(remote(sb.at[q, to[1]], ab.at[q, ex], a_send, a_recv.at[q, d], to))

    def packing(shape, packed_dim):
        r = lax.broadcasted_iota(jnp.int32, shape, packed_dim)
        k = lax.broadcasted_iota(jnp.int32, shape, 1 - packed_dim)
        col = (
            ((r & (TILE - 1)) >> log2(slots)) * rows
            + ((r >> log2(TILE)) << log2(slots)) + (r & (slots - 1))
        )
        return jnp.where(k == col, 1.0, 0.0).astype(BF16)

    pack = packing((packed, parts * rows), 0)
    unpack = packing((parts * rows, packed), 1)

    def gx(q, owner_b, d):
        block = x.at[q, owner_b, lax.rem(za + outer - d, outer)]
        return remote(block, block, gx_send, gx_recv.at[q, d], partner)

    def gz(q, d, owner_a):
        block = x.at[q, xb, owner_a]
        return remote(block, block, gz_send, gz_recv.at[q, d], at_outer(d))

    order = sorted(range(1, outer), key=lambda d: (min(d, outer - d), d))
    for q in range(stages):
        for d in range(1, ne):
            src = lax.rem(ex + ne - d, ne)
            remote(
                sb.at[q, src], ab.at[q, src], a_send, a_recv.at[q, d], at_expert(d)
            ).wait_recv()
        mine = jnp.dot(
            unpack, ab[q].reshape(packed, wide), preferred_element_type=F32
        ).astype(BF16)
        for p in range(parts):
            x[q, xb, za, :, p * wide:(p + 1) * wide] = mine[p * rows:(p + 1) * rows]
        for d in order:
            start(gz(q, d, za))
        if inner > 1:
            start(gx(q, xb, 0))

    terms = 3
    c_id = lax.broadcasted_iota(jnp.int32, (tokens_here, terms * packed), 1)
    n_id = lax.broadcasted_iota(jnp.int32, (tokens_here, terms * packed), 0)
    c_row = c_id & (packed - 1)
    c_slot = ((c_row >> log2(TILE)) << log2(slots)) + (c_row & (slots - 1))
    small[1].wait()
    weight = jnp.zeros((tokens_here, terms * packed), F32)
    for e in range(ne):
        for s in range(slots):
            weight = jnp.where((c_slot == e * slots + s) & (n_id == sel[e, s]), gat[e, s], weight)
    left = weight
    coef = jnp.zeros_like(weight)
    for i in range(terms):
        term = left.astype(BF16).astype(F32)
        coef = jnp.where((c_id >> log2(packed)) == i, term, coef)
        left = left - term
    c_part = (c_row & (TILE - 1)) >> log2(slots)
    for p in range(parts):
        cmb[p] = jnp.where(c_part == p, coef, 0.0).astype(BF16)

    total_rows = inner * outer * rows
    step = min(256, hid.shape[1])

    def arrive(q):
        for d in order:
            gz(q, d, lax.rem(za + outer - d, outer)).wait_recv()
            if inner > 1:
                start(gx(q, xb, d))

    def multiply(q):
        if inner > 1:
            for d in [0] + order:
                gx(q, other, d).wait_recv()
        if q == 0:
            loads[0].wait()
            loads[1].wait()

        @pl.loop(0, hid.shape[1] // step, unroll=True)
        def _(i):
            at = pl.ds(pl.multiple_of(i * step, step), step)
            block = x[q].reshape(total_rows, span)
            g = jnp.dot(block, wg[q * span:(q + 1) * span, at], preferred_element_type=F32)
            u = jnp.dot(block, wu[q * span:(q + 1) * span, at], preferred_element_type=F32)
            if q > 0:
                g = g + g_acc[:, at]
                u = u + u_acc[:, at]
            if q < stages - 1:
                g_acc[:, at] = g
                u_acc[:, at] = u
            else:
                hid[:, at] = (g / (1.0 + jnp.exp(-g)) * u).astype(BF16)

    for q in range(stages):
        arrive(q)
        if q > 0:
            multiply(q - 1)
    multiply(stages - 1)

    loads[2].wait()

    def rx(c):
        return remote(pb.at[c, other], xr.at[c], rx_send, rx_recv.at[c], partner)

    @pl.loop(0, chunks)
    def _(c):
        at = pl.ds(pl.multiple_of(c * cols, cols), cols)
        part = jnp.dot(hid[...], wd[:, at], preferred_element_type=F32)
        pb[c] = part.astype(BF16).reshape(inner, outer, rows, cols)
        if inner > 1:
            rx(c).start()

    def rz(c, d):
        to = lax.rem(za + d, outer)
        return remote(zb.at[c, to], zr.at[c, d - 1], rz_send, rz_recv.at[c, d], at_outer(d))

    def inner_sum(c):
        value = pb[c, xb].astype(F32)
        if inner > 1:
            rx(c).wait_recv()
            value = value + xr[c].astype(F32)
        zb[c] = value.astype(BF16)
        for d in order:
            rz(c, d).start()

    per = span // cols

    def outer_sum(c):
        value = zb[c, za].astype(F32)
        for d in order:
            rz(c, d).wait_recv()
            value = value + zr[c, d - 1].astype(F32)
        for k in range(cols // wide):
            p = (c % per) * (cols // wide) + k
            summed[c // per, p] = value[:, k * wide:(k + 1) * wide].astype(BF16)

    def give(q):
        back = jnp.dot(pack, summed[q].reshape(parts * rows, wide), preferred_element_type=F32)
        rb[q] = back.astype(BF16).reshape(ne, TILE, wide)
        ob[q, ex] = rb[q, ex]
        for d in range(1, ne):
            to = at_expert(d)
            start(remote(rb.at[q, to[1]], ob.at[q, ex], o_send, o_recv.at[q, d], to))

    lag = min(3, chunks)
    for c in range(chunks + lag):
        if c < chunks:
            inner_sum(c)
        done = c - lag
        if done >= 0:
            outer_sum(done)
            if done % per == per - 1:
                give(done // per)

    for q in range(stages):
        for d in range(1, ne):
            src = lax.rem(ex + ne - d, ne)
            remote(
                rb.at[q, src], ob.at[q, src], o_send, o_recv.at[q, d], at_expert(d)
            ).wait_recv()

    def drain(block, sem, to):
        remote(block, block, sem, sem, to).wait_send()

    drain(sb.at[:, 0:ne - 1], a_send, at_expert(1))
    drain(rb.at[:, 0:ne - 1], o_send, at_expert(1))
    if outer > 1:
        drain(x.at[:, 0, 0:outer - 1], gz_send, at_outer(1))
        drain(zb.at[:, 0:outer - 1], rz_send, at_outer(1))
    if inner > 1:
        drain(x.at[:, 0], gx_send, partner)
        drain(pb.at[:, 0], rx_send, partner)


def mix(ob, cmb, out_hbm, out, sem):
    stages, ne, tile, wide = ob.shape
    parts, tokens_here, depth = cmb.shape
    packed = ne * tile
    terms = depth // packed
    span = parts * wide
    stores = []
    for q in range(stages):
        got = ob[q].reshape(packed, wide)
        total = jnp.dot(
            cmb[...].reshape(parts * tokens_here, depth),
            jnp.concatenate([got] * terms, axis=0),
            preferred_element_type=F32,
        ).astype(BF16)
        for p in range(parts):
            at = q * span + p * wide
            out[:, at:at + wide] = total[p * tokens_here:(p + 1) * tokens_here]
        at = pl.ds(q * span, span)
        store = pltpu.make_async_copy(out.at[:, at], out_hbm.at[:, at], sem.at[q])
        store.start()
        stores.append(store)
    for store in stores:
        store.wait()


def per_device(nd, ne, tokens, select, gates, w_gate, w_up, w_down):
    tok_dev, width = tokens.shape
    slots = select.shape[1]
    hidden = w_gate.shape[2]
    inner = 2 if nd % 2 == 0 else 1
    outer = nd // inner
    rows = ne * slots
    parts = TILE // slots
    stages = 4
    span = width // stages
    wide = span // parts
    cols = span // 2
    chunks = width // cols
    vmem = pl.BlockSpec(memory_space=pltpu.VMEM)
    hbm = pl.BlockSpec(memory_space=pl.ANY)
    dma = pltpu.SemaphoreType.DMA
    returned, coef = pl.pallas_call(
        functools.partial(kernel, nd, ne),
        out_shape=(
            pltpu.VMEM((stages, ne, TILE, wide), BF16),
            pltpu.VMEM((parts, tok_dev, 3 * ne * TILE), BF16),
        ),
        in_specs=[hbm] * 6,
        out_specs=(vmem, vmem),
        scratch_shapes=[
            pltpu.VMEM((tok_dev, width), BF16),
            pltpu.SMEM(select.shape, jnp.int32),
            pltpu.SMEM(gates.shape, F32),
            pltpu.VMEM((width, hidden), BF16),
            pltpu.VMEM((width, hidden), BF16),
            pltpu.VMEM((hidden, width), BF16),
            pltpu.VMEM((stages, ne, TILE, wide), BF16),
            pltpu.VMEM((stages, ne, TILE, wide), BF16),
            pltpu.VMEM((stages, inner, outer, rows, span), BF16),
            pltpu.VMEM((nd * rows, hidden), F32),
            pltpu.VMEM((nd * rows, hidden), F32),
            pltpu.VMEM((nd * rows, hidden), BF16),
            pltpu.VMEM((chunks, inner, outer, rows, cols), BF16),
            pltpu.VMEM((chunks, outer, rows, cols), BF16),
            pltpu.VMEM((chunks, outer, rows, cols), BF16),
            pltpu.VMEM((chunks, max(outer - 1, 1), rows, cols), BF16),
            pltpu.VMEM((stages, parts, rows, wide), BF16),
            pltpu.VMEM((stages, ne, TILE, wide), BF16),
            dma(()), dma((2,)),
            dma((3,)),
            dma(()), dma((stages, ne)),
            dma(()), dma((stages, outer)),
            dma(()), dma((stages, outer)),
            dma(()), dma((chunks,)),
            dma(()), dma((chunks, outer)),
            dma(()), dma((stages, ne)),
        ],
        compiler_params=pltpu.CompilerParams(
            collective_id=0, has_side_effects=True, vmem_limit_bytes=60 * 1024 * 1024
        ),
    )(tokens, select, gates, w_gate, w_up, w_down)
    return pl.pallas_call(
        mix,
        out_shape=jax.ShapeDtypeStruct((tok_dev, width), BF16),
        in_specs=[vmem, vmem],
        out_specs=hbm,
        scratch_shapes=[pltpu.VMEM((tok_dev, width), BF16), dma((stages,))],
    )(pltpu.with_memory_space_constraint(returned, pltpu.VMEM), pltpu.with_memory_space_constraint(coef, pltpu.VMEM))


def solution(mesh):
    return jax.shard_map(
        functools.partial(per_device, mesh.shape["dp"], mesh.shape["expert"]),
        mesh=mesh,
        in_specs=(
            P(("dp", "expert"), None),
            P(None, ("dp", "expert")),
            P(None, ("dp", "expert")),
            P("expert", None, "dp"),
            P("expert", None, "dp"),
            P("expert", "dp", None),
        ),
        out_specs=P(("dp", "expert"), None),
        check_vma=False,
    )
```

```python
import functools

import jax
import jax.numpy as jnp
from jax import lax
from jax.experimental import pallas as pl
from jax.experimental.pallas import tpu as pltpu
from jax.sharding import PartitionSpec as P

MESH = pl.DeviceIdType.MESH
TILE = 16
F32 = jnp.float32
BF16 = jnp.bfloat16
scope = jax.named_scope


def log2(n):
    return n.bit_length() - 1


def kernel(
    nd, ne, tok_hbm, sel_hbm, gat_hbm, wg_hbm, wu_hbm, wd_hbm, ob, cmb,
    tok, sel, gat, wg, wu, wd, sb, xp, unp, xs, g_acc, u_acc, hid, pb, xr, zb, zr, summed, rb,
    l_sem, w_sem, a_send, a_recv, gz_send, gf_send, gz_recv, gx_send, gx_recv,
    rx_send, rx_recv, rz_send, rz_recv, o_send, o_recv,
):
    batches, stages, inner, outer, each, _, wide = xp.shape
    slots = sel.shape[1]
    tokens_here = tok.shape[0]
    parts = TILE // slots
    span = wide * parts
    rows = each * slots
    chunks = pb.shape[1]
    tile_rows, tile_cols = pb.shape[4:]
    fold = tile_rows // rows
    cols = fold * tile_cols
    units = ob.shape[0]
    per = chunks // units
    packed = ne * TILE
    total_rows = inner * outer * rows
    half = outer // 2
    pair = 2 if ne % 2 == 0 else 1
    chips = ne // pair
    dp = lax.axis_index("dp")
    ex = lax.axis_index("expert")
    za = dp // inner
    xb = lax.rem(dp, inner)
    other = (inner - 1) - xb
    chip = ex // pair
    core = lax.rem(ex, pair)

    def at_expert(t):
        to_chip = lax.rem(chip + t // pair, chips)
        return to_chip * pair + lax.rem(core + t % pair, pair)

    def at_z(z):
        return (z * inner + xb, ex)

    def at_outer(d):
        return at_z(lax.rem(za + d, outer))

    partner = (za * inner + other, ex)

    def remote(src, dst, send, recv, to):
        return pltpu.make_async_remote_copy(
            src_ref=src, dst_ref=dst, send_sem=send, recv_sem=recv,
            device_id=to, device_id_type=MESH,
        )

    fetch = pltpu.make_async_copy(tok_hbm, tok, l_sem.at[0])
    fetch.start()
    get_sel = pltpu.make_async_copy(sel_hbm, sel, l_sem.at[1])
    get_sel.start()
    get_gat = pltpu.make_async_copy(gat_hbm, gat, l_sem.at[2])
    get_gat.start()
    barrier = pltpu.get_barrier_semaphore()
    for t in range(1, ne):
        pl.semaphore_signal(barrier, inc=1, device_id=(dp, at_expert(t)), device_id_type=MESH)
    for d in range(1, outer):
        pl.semaphore_signal(barrier, inc=1, device_id=at_outer(d), device_id_type=MESH)
    if inner > 1:
        pl.semaphore_signal(barrier, inc=1, device_id=partner, device_id_type=MESH)

    get_sel.wait()
    r_id = lax.broadcasted_iota(jnp.int32, (packed, tokens_here), 0)
    t_id = lax.broadcasted_iota(jnp.int32, (packed, tokens_here), 1)
    r_slot = ((r_id >> log2(TILE)) << log2(slots)) + (r_id & (slots - 1))
    r_part = (r_id & (TILE - 1)) >> log2(slots)
    named = jnp.full((packed, tokens_here), -1, jnp.int32)
    for e in range(ne):
        for s in range(slots):
            named = jnp.where(r_slot == e * slots + s, sel[e, s], named)
    hit = jnp.where(named == t_id, 1.0, 0.0)
    pick = jnp.concatenate(
        [jnp.where(r_part == p, hit, 0.0).astype(BF16) for p in range(parts)], axis=1
    )
    with scope("fetch"):
        fetch.wait()
    loads = [
        pltpu.make_async_copy(h.at[0], v, w_sem.at[i])
        for i, (h, v) in enumerate(((wg_hbm, wg), (wu_hbm, wu), (wd_hbm, wd)))
    ]
    for load in loads:
        load.start()

    def place(e, j):
        r = lax.rem(j - (e // pair) * pair + ne, ne)
        return r // each, lax.rem(r, each)

    mine = place(ex, ex)[1]
    for q in range(stages):
        stack = jnp.concatenate(
            [tok[:, q * span + p * wide:q * span + (p + 1) * wide] for p in range(parts)], axis=0
        )
        gathered = jnp.dot(pick, stack, preferred_element_type=F32).astype(BF16)
        sb[q] = gathered.reshape(ne, TILE, wide)
        xp[0, q, xb, za, mine] = sb[q, ex]

    with scope("barrier"):
        pl.semaphore_wait(barrier, (ne - 1) + (outer - 1) + (1 if inner > 1 else 0))

    for t in range(1, ne):
        for q in range(stages):
            e = at_expert(t)
            b, k = place(e, ex)
            remote(
                sb.at[q, e], xp.at[b, q, xb, za, k], a_send, a_recv.at[b, q], (dp, e)
            ).start()

    relayed = outer >= 4 and outer % 2 == 0
    my_half = za // max(half, 1)
    near_gate = half - 1 + my_half
    far_gate = half - my_half

    def is_relayed(b, q):
        return relayed and RELAY[b]

    def targets(b, q):
        if not is_relayed(b, q):
            return [lax.rem(za + d, outer) for d in sorted(range(1, outer), key=lambda d: min(d, outer - d))]
        mates = [my_half * half + lax.rem(za - my_half * half + i, half) for i in range(1, half)]
        return mates + [far_gate]

    def send_own(b, q, k, n):
        block = xp.at[b, q, xb, za, pl.ds(k, n)]
        if inner > 1:
            remote(block, block, gx_send, gx_recv.at[b, q], partner).start()
        for z in targets(b, q):
            remote(block, block, gz_send.at[b], gz_recv.at[b, q, za], at_z(z)).start()

    def own_first(q):
        send_own(0, q, mine, 1)

    def own(b, q):
        arrived = xp.at[b, q, xb, za, pl.ds(0, each - 1 if b == 0 else each)]
        if b > 0:
            remote(arrived, arrived, a_send, a_recv.at[b, q], partner).wait_recv()
            send_own(b, q, 0, each)
        elif each > 1:
            remote(arrived, arrived, a_send, a_recv.at[b, q], partner).wait_recv()
            for i in range(1, each):
                send_own(b, q, lax.rem(mine + i, each), 1)

    def take(b, q, z):
        block = xp.at[b, q, xb, z]
        remote(block, block, gz_send.at[b], gz_recv.at[b, q, z], partner).wait_recv()
        if inner > 1:
            remote(block, block, gx_send, gx_recv.at[b, q], partner).start()

    def mate(i):
        return my_half * half + lax.rem(za - my_half * half + i, half)

    def arrive(b, q):
        if not is_relayed(b, q):
            for d in sorted(range(1, outer), key=lambda d: min(d, outer - d)):
                take(b, q, lax.rem(za + outer - d, outer))
            return
        for i in range(1, half):
            take(b, q, mate(i))

    def far_side():
        return [far_gate + i * (1 - 2 * my_half) for i in range(half)]

    def relay(b, q):
        if not is_relayed(b, q):
            return

        @pl.when(za == near_gate)
        def _():
            for z in far_side():
                take(b, q, z)
                block = xp.at[b, q, xb, z]
                for i in range(1, half):
                    remote(
                        block, block, gf_send.at[b, i - 1], gz_recv.at[b, q, z], at_z(mate(i))
                    ).start()

    def distant(b, q):
        if not is_relayed(b, q):
            return

        @pl.when(za != near_gate)
        def _():
            for z in far_side():
                take(b, q, z)

    def spread():
        r = lax.broadcasted_iota(jnp.int32, unp.shape, 0)
        k = lax.broadcasted_iota(jnp.int32, unp.shape, 1)
        part = r >> log2(total_rows)
        row = r & (total_rows - 1)
        col = ((row >> log2(slots)) << log2(TILE)) + (part << log2(slots)) + (row & (slots - 1))
        unp[...] = jnp.where(k == col, 1.0, 0.0).astype(BF16)

    step = min(256, hid.shape[1])
    blocks = hid.shape[1] // step

    def ready(b, q):
        if inner > 1:
            block = xp.at[b, q, other]
            remote(block, block, gx_send, gx_recv.at[b, q], partner).wait_recv()
        if b == 0 and q == 0:
            loads[0].wait()
            loads[1].wait()
        flat = jnp.dot(
            unp[...], xp[b, q].reshape(parts * total_rows, wide), preferred_element_type=F32
        ).astype(BF16)
        for p in range(parts):
            xs[:, p * wide:(p + 1) * wide] = flat[p * total_rows:(p + 1) * total_rows]

    def multiply(b, q, i):
        at = pl.ds(i * step, step)
        g = jnp.dot(xs[...], wg[q * span:(q + 1) * span, at], preferred_element_type=F32)
        u = jnp.dot(xs[...], wu[q * span:(q + 1) * span, at], preferred_element_type=F32)
        if q > 0:
            g = g + g_acc[:, at]
            u = u + u_acc[:, at]
        if q < stages - 1:
            g_acc[:, at] = g
            u_acc[:, at] = u
        else:
            hid[:, at] = (g / (1.0 + jnp.exp(-g)) * u).astype(BF16)

    def rx(b, c):
        return remote(pb.at[b, c, other], xr.at[b, c], rx_send, rx_recv.at[b, c], partner)

    def down(b, c):
        if b == 0 and c == 0:
            loads[2].wait()
        at = pl.ds(c * cols, cols)
        part = jnp.dot(hid[...], wd[:, at], preferred_element_type=F32)
        part = part.reshape(inner, outer, rows, cols)
        part = jnp.concatenate(
            [part[..., f * tile_cols:(f + 1) * tile_cols] for f in range(fold)], axis=2
        )
        pb[b, c] = part.astype(BF16)
        if inner > 1:
            rx(b, c).start()

    def inner_sum(b, c):
        value = pb[b, c, xb].astype(F32)
        if inner > 1:
            rx(b, c).wait_recv()
            value = value + xr[b, c].astype(F32)
        zb[b, c] = value.astype(BF16)
        for d in sorted(range(1, outer), key=lambda d: -min(d, outer - d)):
            to = lax.rem(za + d, outer)
            remote(
                zb.at[b, c, to], zr.at[b, c, d - 1], rz_send, rz_recv.at[b, c], at_z(to)
            ).start()

    def packing():
        r = lax.broadcasted_iota(jnp.int32, (each * TILE, parts * rows), 0)
        k = lax.broadcasted_iota(jnp.int32, (each * TILE, parts * rows), 1)
        col = (
            ((r & (TILE - 1)) >> log2(slots)) * rows
            + ((r >> log2(TILE)) << log2(slots)) + (r & (slots - 1))
        )
        return jnp.where(k == col, 1.0, 0.0).astype(BF16)

    def outer_sum(b, c):
        value = zb[b, c, za].astype(F32)
        if outer > 1:
            remote(zr.at[b, c], zr.at[b, c], rz_send, rz_recv.at[b, c], partner).wait_recv()
            for d in range(1, outer):
                value = value + zr[b, c, d - 1].astype(F32)
        unit, i = c // per, c % per
        summed[b, unit, i * tile_rows:(i + 1) * tile_rows] = value.astype(BF16)
        if i == per - 1:
            give(b, unit)

    def give(b, unit):
        back = jnp.dot(packing(), summed[b, unit], preferred_element_type=F32)
        rb[b, unit] = back.astype(BF16).reshape(each, TILE, wide)
        if b == 0:
            ob[unit, ex] = rb[b, unit, mine]
            ks = [lax.rem(mine + i, each) for i in range(1, each)]
        else:
            ks = list(range(each))
        for k in ks:
            j = lax.rem(chip * pair + b * each + k, ne)
            remote(rb.at[b, unit, k], ob.at[unit, ex], o_send, o_recv, (dp, j)).start()

    def weigh():
        get_gat.wait()
        terms = 3
        c_id = lax.broadcasted_iota(jnp.int32, (tokens_here, terms * packed), 1)
        n_id = lax.broadcasted_iota(jnp.int32, (tokens_here, terms * packed), 0)
        c_row = c_id & (packed - 1)
        c_slot = ((c_row >> log2(TILE)) << log2(slots)) + (c_row & (slots - 1))
        weight = jnp.zeros((tokens_here, terms * packed), F32)
        for e in range(ne):
            for s in range(slots):
                weight = jnp.where(
                    (c_slot == e * slots + s) & (n_id == sel[e, s]), gat[e, s], weight
                )
        left = weight
        coef = jnp.zeros_like(weight)
        for i in range(terms):
            term = left.astype(BF16).astype(F32)
            coef = jnp.where((c_id >> log2(packed)) == i, term, coef)
            left = left - term
        c_part = (c_row & (TILE - 1)) >> log2(slots)
        for p in range(parts):
            cmb[p] = jnp.where(c_part == p, coef, 0.0).astype(BF16)

    tasks = dict(
        first=own_first, own=own, arrive=arrive, relay=relay, distant=distant, spread=spread, ready=ready, mult=multiply,
        down=down, inner=inner_sum, outer=outer_sum, weigh=weigh,
    )
    for name, *args in order(batches, stages, blocks, chunks):
        with scope("_".join([name] + [str(a) for a in args])):
            tasks[name](*args)

    def drain(block, sem):
        remote(block, block, sem, sem, partner).wait_send()

    with scope("back"):
        landed = ob.at[:, 0:ne - 1]
        remote(landed, landed, o_send, o_recv, partner).wait_recv()
    drain(sb.at[:, 0:ne - 1], a_send)
    drain(landed, o_send)
    if outer > 1:
        drain(zb.at[:, :, 0:outer - 1], rz_send)
        for b in range(batches):
            relay = is_relayed(b, 0)
            drain(xp.at[b, :, 0, 0:half if relay else outer - 1], gz_send.at[b])
            if relay:
                @pl.when(za == near_gate)
                def _():
                    for i in range(half - 1):
                        drain(xp.at[b, :, 0, 0:half], gf_send.at[b, i])
    if inner > 1:
        drain(xp.at[:, :, 0], gx_send)
        drain(pb.at[:, :, 0], rx_send)


RELAY = (False, True)


def order(batches, stages, blocks, chunks):
    last = batches - 1
    both = range(batches)
    yield from (("first", q) for q in range(stages))
    yield ("spread",)
    for b in both:
        yield from (("own", b, q) for q in range(stages))
    for q in range(stages):
        yield ("arrive", 0, q)
        yield ("relay", 0, q)
        if last:
            yield ("arrive", 1, q)
    yield from (("distant", 0, q) for q in range(stages))
    yield ("weigh",)
    for q in range(stages):
        if last:
            yield ("relay", 1, q)
        yield ("ready", 0, q)
        for i in range(blocks):
            yield ("mult", 0, q, i)
            if last and q > 0 and i == 1:
                yield ("distant", 1, 0)
    for c in range(chunks):
        yield ("down", 0, c)
        if last and c < stages - 1:
            yield ("distant", 1, c + 1)
    n = 0
    if last:
        for q in range(stages):
            yield ("ready", 1, q)
            for i in range(blocks):
                yield ("mult", 1, q, i)
                if q > 0 and i % 2 == 1 and n < chunks:
                    yield ("inner", 0, n)
                    n += 1
        for c in range(chunks):
            yield ("down", 1, c)
            if c % 2 == 1 and n < chunks:
                yield ("inner", 0, n)
                n += 1
    for c in range(n, chunks):
        yield ("inner", 0, c)
    lag = 1
    for c in range(chunks + lag):
        if last and c < chunks:
            yield ("inner", 1, c)
        if c >= lag:
            yield ("outer", 0, c - lag)
    if last:
        yield from (("outer", 1, c) for c in range(chunks))


def mix(ob, cmb, out_hbm, out, sem):
    stages, ne, tile, wide = ob.shape
    parts, tokens_here, depth = cmb.shape
    packed = ne * tile
    terms = depth // packed
    span = parts * wide
    stores = []
    for q in range(stages):
        got = ob[q].reshape(packed, wide)
        total = jnp.dot(
            cmb[...].reshape(parts * tokens_here, depth),
            jnp.concatenate([got] * terms, axis=0),
            preferred_element_type=F32,
        ).astype(BF16)
        for p in range(parts):
            at = q * span + p * wide
            out[:, at:at + wide] = total[p * tokens_here:(p + 1) * tokens_here]
        at = pl.ds(q * span, span)
        store = pltpu.make_async_copy(out.at[:, at], out_hbm.at[:, at], sem.at[q])
        store.start()
        stores.append(store)
    for store in stores:
        store.wait()


def per_device(nd, ne, tokens, select, gates, w_gate, w_up, w_down):
    tok_dev, width = tokens.shape
    slots = select.shape[1]
    hidden = w_gate.shape[2]
    inner = 2 if nd % 2 == 0 else 1
    outer = nd // inner
    parts = TILE // slots
    batches = 2 if ne % 2 == 0 and (ne // 2 * slots) % 8 == 0 else 1
    each = ne // batches
    rows = each * slots
    stages = 2
    span = width // stages
    wide = span // parts
    fold = max(1, TILE // rows)
    tile_rows = fold * rows
    chunks = width // (fold * wide)
    total_rows = nd * rows
    vmem = pl.BlockSpec(memory_space=pltpu.VMEM)
    hbm = pl.BlockSpec(memory_space=pl.ANY)
    dma = pltpu.SemaphoreType.DMA
    returned, coef = pl.pallas_call(
        functools.partial(kernel, nd, ne),
        out_shape=(
            pltpu.VMEM((stages, ne, TILE, wide), BF16),
            pltpu.VMEM((parts, tok_dev, 3 * ne * TILE), BF16),
        ),
        in_specs=[hbm] * 6,
        out_specs=(vmem, vmem),
        scratch_shapes=[
            pltpu.VMEM((tok_dev, width), BF16),
            pltpu.SMEM(select.shape, jnp.int32),
            pltpu.SMEM(gates.shape, F32),
            pltpu.VMEM((width, hidden), BF16),
            pltpu.VMEM((width, hidden), BF16),
            pltpu.VMEM((hidden, width), BF16),
            pltpu.VMEM((stages, ne, TILE, wide), BF16),
            pltpu.VMEM((batches, stages, inner, outer, each, TILE, wide), BF16),
            pltpu.VMEM((parts * total_rows, parts * total_rows), BF16),
            pltpu.VMEM((total_rows, span), BF16),
            pltpu.VMEM((total_rows, hidden), F32),
            pltpu.VMEM((total_rows, hidden), F32),
            pltpu.VMEM((total_rows, hidden), BF16),
            pltpu.VMEM((batches, chunks, inner, outer, tile_rows, wide), BF16),
            pltpu.VMEM((batches, chunks, outer, tile_rows, wide), BF16),
            pltpu.VMEM((batches, chunks, outer, tile_rows, wide), BF16),
            pltpu.VMEM((batches, chunks, max(outer - 1, 1), tile_rows, wide), BF16),
            pltpu.VMEM((batches, stages, parts * rows, wide), BF16),
            pltpu.VMEM((batches, stages, each, TILE, wide), BF16),
            dma((3,)), dma((3,)),
            dma(()), dma((batches, stages)),
            dma((batches,)), dma((batches, max(outer // 2 - 1, 1))),
            dma((batches, stages, outer)),
            dma(()), dma((batches, stages)),
            dma(()), dma((batches, chunks)),
            dma(()), dma((batches, chunks)),
            dma(()), dma(()),
        ],
        compiler_params=pltpu.CompilerParams(
            collective_id=0, has_side_effects=True, vmem_limit_bytes=60 * 1024 * 1024
        ),
    )(tokens, select, gates, w_gate, w_up, w_down)
    return pl.pallas_call(
        mix,
        out_shape=jax.ShapeDtypeStruct((tok_dev, width), BF16),
        in_specs=[vmem, vmem],
        out_specs=hbm,
        scratch_shapes=[pltpu.VMEM((tok_dev, width), BF16), dma((stages,))],
    )(
        pltpu.with_memory_space_constraint(returned, pltpu.VMEM),
        pltpu.with_memory_space_constraint(coef, pltpu.VMEM),
    )


def solution(mesh):
    return jax.shard_map(
        functools.partial(per_device, mesh.shape["dp"], mesh.shape["expert"]),
        mesh=mesh,
        in_specs=(
            P(("dp", "expert"), None),
            P(None, ("dp", "expert")),
            P(None, ("dp", "expert")),
            P("expert", None, "dp"),
            P("expert", None, "dp"),
            P("expert", "dp", None),
        ),
        out_specs=P(("dp", "expert"), None),
        check_vma=False,
    )
```

```python
import functools

import jax
import jax.numpy as jnp
from jax import lax
from jax.experimental import pallas as pl
from jax.experimental.pallas import tpu as pltpu
from jax.sharding import PartitionSpec as P

MESH = pl.DeviceIdType.MESH
TILE = 16
F32 = jnp.float32
BF16 = jnp.bfloat16
scope = jax.named_scope


def log2(n):
    return n.bit_length() - 1


def kernel(
    nd, ne, tok_hbm, sel_hbm, gat_hbm, wg_hbm, wu_hbm, wd_hbm, ob, cmb,
    tok, sel, gat, wg, wu, wd, sb, xp, unp, xs, g_acc, u_acc, hid, pb, xr, zb, zr, summed, rb,
    l_sem, w_sem, a_send, a_recv, gz_send, gf_send, gz_recv, gx_send, gx_recv,
    rx_send, rx_recv, rz_send, rz_recv, o_send, o_recv,
):
    batches, stages, inner, outer, each, _, wide = xp.shape
    slots = sel.shape[1]
    tokens_here = tok.shape[0]
    parts = TILE // slots
    span = wide * parts
    rows = each * slots
    chunks = pb.shape[1]
    tile_rows, tile_cols = pb.shape[4:]
    fold = tile_rows // rows
    cols = fold * tile_cols
    units = ob.shape[0]
    per = chunks // units
    packed = ne * TILE
    total_rows = inner * outer * rows
    half = outer // 2
    pair = 2 if ne % 2 == 0 else 1
    chips = ne // pair
    dp = lax.axis_index("dp")
    ex = lax.axis_index("expert")
    za = dp // inner
    xb = lax.rem(dp, inner)
    other = (inner - 1) - xb
    chip = ex // pair
    core = lax.rem(ex, pair)

    def at_expert(t):
        to_chip = lax.rem(chip + t // pair, chips)
        return to_chip * pair + lax.rem(core + t % pair, pair)

    def at_z(z):
        return (z * inner + xb, ex)

    def at_outer(d):
        return at_z(lax.rem(za + d, outer))

    partner = (za * inner + other, ex)

    def remote(src, dst, send, recv, to):
        return pltpu.make_async_remote_copy(
            src_ref=src, dst_ref=dst, send_sem=send, recv_sem=recv,
            device_id=to, device_id_type=MESH,
        )

    fetch = pltpu.make_async_copy(tok_hbm, tok, l_sem.at[0])
    fetch.start()
    get_sel = pltpu.make_async_copy(sel_hbm, sel, l_sem.at[1])
    get_sel.start()
    get_gat = pltpu.make_async_copy(gat_hbm, gat, l_sem.at[2])
    get_gat.start()
    barrier = pltpu.get_barrier_semaphore()
    for t in range(1, ne):
        pl.semaphore_signal(barrier, inc=1, device_id=(dp, at_expert(t)), device_id_type=MESH)
    for d in range(1, outer):
        pl.semaphore_signal(barrier, inc=1, device_id=at_outer(d), device_id_type=MESH)
    if inner > 1:
        pl.semaphore_signal(barrier, inc=1, device_id=partner, device_id_type=MESH)

    get_sel.wait()
    r_id = lax.broadcasted_iota(jnp.int32, (packed, tokens_here), 0)
    t_id = lax.broadcasted_iota(jnp.int32, (packed, tokens_here), 1)
    r_slot = ((r_id >> log2(TILE)) << log2(slots)) + (r_id & (slots - 1))
    r_part = (r_id & (TILE - 1)) >> log2(slots)
    named = jnp.full((packed, tokens_here), -1, jnp.int32)
    for e in range(ne):
        for s in range(slots):
            named = jnp.where(r_slot == e * slots + s, sel[e, s], named)
    hit = jnp.where(named == t_id, 1.0, 0.0)
    pick = jnp.concatenate(
        [jnp.where(r_part == p, hit, 0.0).astype(BF16) for p in range(parts)], axis=1
    )
    with scope("fetch"):
        fetch.wait()
    loads = [
        pltpu.make_async_copy(h.at[0], v, w_sem.at[i])
        for i, (h, v) in enumerate(((wg_hbm, wg), (wu_hbm, wu), (wd_hbm, wd)))
    ]
    for load in loads:
        load.start()

    def place(e, j):
        r = lax.rem(j - (e // pair) * pair + ne, ne)
        return r // each, lax.rem(r, each)

    mine = place(ex, ex)[1]
    for q in range(stages):
        stack = jnp.concatenate(
            [tok[:, q * span + p * wide:q * span + (p + 1) * wide] for p in range(parts)], axis=0
        )
        gathered = jnp.dot(pick, stack, preferred_element_type=F32).astype(BF16)
        sb[q] = gathered.reshape(ne, TILE, wide)
        xp[0, q, xb, za, mine] = sb[q, ex]

    with scope("barrier"):
        pl.semaphore_wait(barrier, (ne - 1) + (outer - 1) + (1 if inner > 1 else 0))

    for t in range(1, ne):
        for q in range(stages):
            e = at_expert(t)
            b, k = place(e, ex)
            remote(
                sb.at[q, e], xp.at[b, q, xb, za, k], a_send, a_recv.at[b, q], (dp, e)
            ).start()

    relayed = outer >= 4 and outer % 2 == 0 and pair > 1
    my_half = za // max(half, 1)
    near_gate = half - 1 + my_half
    far_gate = half - my_half

    relays = core == pair - 1
    near = sorted(range(1, outer), key=lambda d: min(d, outer - d))

    def mate(i):
        return my_half * half + lax.rem(za - my_half * half + i, half)

    def far_side():
        return [far_gate + i * (1 - 2 * my_half) for i in range(half)]

    def send_own(b, q, k, n):
        block = xp.at[b, q, xb, za, pl.ds(k, n)]
        if inner > 1:
            remote(block, block, gx_send, gx_recv.at[b, q], partner).start()

        def send(z):
            remote(block, block, gz_send.at[b], gz_recv.at[b, q, za], at_z(z)).start()

        if not relayed:
            for d in near:
                send(lax.rem(za + d, outer))
            return
        for i in range(1, half):
            send(mate(i))

        @pl.when(relays)
        def _():
            send(far_gate)

        @pl.when(jnp.logical_not(relays))
        def _():
            for z in far_side():
                send(z)

    def own_first(q):
        send_own(0, q, mine, 1)

    def own(b, q):
        arrived = xp.at[b, q, xb, za, pl.ds(0, each - 1 if b == 0 else each)]
        if b > 0:
            remote(arrived, arrived, a_send, a_recv.at[b, q], partner).wait_recv()
            send_own(b, q, 0, each)
        elif each > 1:
            remote(arrived, arrived, a_send, a_recv.at[b, q], partner).wait_recv()
            for i in range(1, each):
                send_own(b, q, lax.rem(mine + i, each), 1)

    def take(b, q, z):
        block = xp.at[b, q, xb, z]
        remote(block, block, gz_send.at[b], gz_recv.at[b, q, z], partner).wait_recv()
        if inner > 1:
            remote(block, block, gx_send, gx_recv.at[b, q], partner).start()

    def arrive(b, q):
        if not relayed:
            for d in near:
                take(b, q, lax.rem(za + outer - d, outer))
            return
        for i in range(1, half):
            take(b, q, mate(i))

    def relay(b, q):
        if not relayed:
            return

        @pl.when(relays & (za == near_gate))
        def _():
            for z in far_side():
                take(b, q, z)
                block = xp.at[b, q, xb, z]
                for i in range(1, half):
                    remote(
                        block, block, gf_send.at[b, i - 1], gz_recv.at[b, q, z], at_z(mate(i))
                    ).start()

    def distant(b, q):
        if not relayed:
            return

        @pl.when(jnp.logical_not(relays & (za == near_gate)))
        def _():
            for z in far_side():
                take(b, q, z)

    def spread():
        r = lax.broadcasted_iota(jnp.int32, unp.shape, 0)
        k = lax.broadcasted_iota(jnp.int32, unp.shape, 1)
        part = r >> log2(total_rows)
        row = r & (total_rows - 1)
        col = ((row >> log2(slots)) << log2(TILE)) + (part << log2(slots)) + (row & (slots - 1))
        unp[...] = jnp.where(k == col, 1.0, 0.0).astype(BF16)

    step = min(256, hid.shape[1])
    blocks = hid.shape[1] // step

    def ready(b, q):
        if inner > 1:
            block = xp.at[b, q, other]
            remote(block, block, gx_send, gx_recv.at[b, q], partner).wait_recv()
        if b == 0 and q == 0:
            loads[0].wait()
            loads[1].wait()
        flat = jnp.dot(
            unp[...], xp[b, q].reshape(parts * total_rows, wide), preferred_element_type=F32
        ).astype(BF16)
        for p in range(parts):
            xs[:, p * wide:(p + 1) * wide] = flat[p * total_rows:(p + 1) * total_rows]

    def multiply(b, q, i):
        at = pl.ds(i * step, step)
        g = jnp.dot(xs[...], wg[q * span:(q + 1) * span, at], preferred_element_type=F32)
        u = jnp.dot(xs[...], wu[q * span:(q + 1) * span, at], preferred_element_type=F32)
        if q > 0:
            g = g + g_acc[:, at]
            u = u + u_acc[:, at]
        if q < stages - 1:
            g_acc[:, at] = g
            u_acc[:, at] = u
        else:
            hid[:, at] = (g / (1.0 + jnp.exp(-g)) * u).astype(BF16)

    def rx(b, c):
        return remote(pb.at[b, c, other], xr.at[b, c], rx_send, rx_recv.at[b, c], partner)

    def down(b, c):
        if b == 0 and c == 0:
            loads[2].wait()
        at = pl.ds(c * cols, cols)
        part = jnp.dot(hid[...], wd[:, at], preferred_element_type=F32)
        part = part.reshape(inner, outer, rows, cols)
        part = jnp.concatenate(
            [part[..., f * tile_cols:(f + 1) * tile_cols] for f in range(fold)], axis=2
        )
        pb[b, c] = part.astype(BF16)
        if inner > 1:
            rx(b, c).start()

    def inner_sum(b, c):
        value = pb[b, c, xb].astype(F32)
        if inner > 1:
            rx(b, c).wait_recv()
            value = value + xr[b, c].astype(F32)
        zb[b, c] = value.astype(BF16)
        if relayed:
            order_z = far_side()[::-1] + [mate(i) for i in range(1, half)]
        else:
            order_z = [lax.rem(za + d, outer) for d in near[::-1]]
        for to in order_z:
            slot = lax.rem(to - za + outer, outer) - 1
            remote(
                zb.at[b, c, to], zr.at[b, c, slot], rz_send, rz_recv.at[b, c], at_z(to)
            ).start()

    def packing():
        r = lax.broadcasted_iota(jnp.int32, (each * TILE, parts * rows), 0)
        k = lax.broadcasted_iota(jnp.int32, (each * TILE, parts * rows), 1)
        col = (
            ((r & (TILE - 1)) >> log2(slots)) * rows
            + ((r >> log2(TILE)) << log2(slots)) + (r & (slots - 1))
        )
        return jnp.where(k == col, 1.0, 0.0).astype(BF16)

    def outer_sum(b, c):
        value = zb[b, c, za].astype(F32)
        if outer > 1:
            remote(zr.at[b, c], zr.at[b, c], rz_send, rz_recv.at[b, c], partner).wait_recv()
            for d in range(1, outer):
                value = value + zr[b, c, d - 1].astype(F32)
        unit, i = c // per, c % per
        summed[b, unit, i * tile_rows:(i + 1) * tile_rows] = value.astype(BF16)
        if i == per - 1:
            give(b, unit)

    def give(b, unit):
        back = jnp.dot(packing(), summed[b, unit], preferred_element_type=F32)
        rb[b, unit] = back.astype(BF16).reshape(each, TILE, wide)
        if b == 0:
            ob[unit, ex] = rb[b, unit, mine]
            ks = [lax.rem(mine + i, each) for i in range(1, each)]
        else:
            ks = list(range(each))
        for k in ks:
            j = lax.rem(chip * pair + b * each + k, ne)
            remote(rb.at[b, unit, k], ob.at[unit, ex], o_send, o_recv, (dp, j)).start()

    def weigh():
        get_gat.wait()
        terms = 3
        c_id = lax.broadcasted_iota(jnp.int32, (tokens_here, terms * packed), 1)
        n_id = lax.broadcasted_iota(jnp.int32, (tokens_here, terms * packed), 0)
        c_row = c_id & (packed - 1)
        c_slot = ((c_row >> log2(TILE)) << log2(slots)) + (c_row & (slots - 1))
        weight = jnp.zeros((tokens_here, terms * packed), F32)
        for e in range(ne):
            for s in range(slots):
                weight = jnp.where(
                    (c_slot == e * slots + s) & (n_id == sel[e, s]), gat[e, s], weight
                )
        left = weight
        coef = jnp.zeros_like(weight)
        for i in range(terms):
            term = left.astype(BF16).astype(F32)
            coef = jnp.where((c_id >> log2(packed)) == i, term, coef)
            left = left - term
        c_part = (c_row & (TILE - 1)) >> log2(slots)
        for p in range(parts):
            cmb[p] = jnp.where(c_part == p, coef, 0.0).astype(BF16)

    tasks = dict(
        first=own_first, own=own, arrive=arrive, relay=relay, distant=distant, spread=spread, ready=ready, mult=multiply,
        down=down, inner=inner_sum, outer=outer_sum, weigh=weigh,
    )
    for name, *args in order(batches, stages, blocks, chunks):
        with scope("_".join([name] + [str(a) for a in args])):
            tasks[name](*args)

    def drain(block, sem):
        remote(block, block, sem, sem, partner).wait_send()

    with scope("back"):
        landed = ob.at[:, 0:ne - 1]
        remote(landed, landed, o_send, o_recv, partner).wait_recv()
    drain(sb.at[:, 0:ne - 1], a_send)
    drain(landed, o_send)
    if outer > 1:
        drain(zb.at[:, :, 0:outer - 1], rz_send)
        if not relayed:
            for b in range(batches):
                drain(xp.at[b, :, 0, 0:outer - 1], gz_send.at[b])
        else:
            @pl.when(relays)
            def _():
                for b in range(batches):
                    drain(xp.at[b, :, 0, 0:half], gz_send.at[b])

            @pl.when(jnp.logical_not(relays))
            def _():
                for b in range(batches):
                    drain(xp.at[b, :, 0, 0:outer - 1], gz_send.at[b])

            @pl.when(relays & (za == near_gate))
            def _():
                for b in range(batches):
                    for i in range(half - 1):
                        drain(xp.at[b, :, 0, 0:half], gf_send.at[b, i])
    if inner > 1:
        drain(xp.at[:, :, 0], gx_send)
        drain(pb.at[:, :, 0], rx_send)


def order(batches, stages, blocks, chunks):
    last = batches - 1
    both = range(batches)
    for q in range(stages):
        yield ("first", q)
        yield ("own", 0, q)
    yield ("spread",)
    if last:
        yield from (("own", 1, q) for q in range(stages))
    for q in range(stages):
        yield ("arrive", 0, q)
        yield ("relay", 0, q)
    yield from (("distant", 0, q) for q in range(stages))
    if last:
        yield from (("arrive", 1, q) for q in range(stages))
    yield ("weigh",)
    for q in range(stages):
        if last:
            yield ("relay", 1, q)
        yield ("ready", 0, q)
        for i in range(blocks):
            yield ("mult", 0, q, i)
        if last:
            yield ("distant", 1, q)
    n = 0
    if last:
        yield ("down", 0, 0)
        yield ("down", 0, 1)
        for q in range(stages):
            yield ("ready", 1, q)
            for i in range(blocks):
                yield ("mult", 1, q, i)
                if q == 0 and i % 2 == 1:
                    yield ("down", 0, 2 + i // 2)
                if q > 0 and i % 2 == 1 and n < chunks:
                    yield ("inner", 0, n)
                    n += 1
        for c in range(chunks):
            yield ("down", 1, c)
            if c % 2 == 1 and n < chunks:
                yield ("inner", 0, n)
                n += 1
    for c in range(n, chunks):
        yield ("inner", 0, c)
    lag = 1
    for c in range(chunks + lag):
        if last and c < chunks:
            yield ("inner", 1, c)
        if c >= lag:
            yield ("outer", 0, c - lag)
    if last:
        yield from (("outer", 1, c) for c in range(chunks))


def mix(ob, cmb, out_hbm, out, sem):
    stages, ne, tile, wide = ob.shape
    parts, tokens_here, depth = cmb.shape
    packed = ne * tile
    terms = depth // packed
    span = parts * wide
    stores = []
    for q in range(stages):
        got = ob[q].reshape(packed, wide)
        total = jnp.dot(
            cmb[...].reshape(parts * tokens_here, depth),
            jnp.concatenate([got] * terms, axis=0),
            preferred_element_type=F32,
        ).astype(BF16)
        for p in range(parts):
            at = q * span + p * wide
            out[:, at:at + wide] = total[p * tokens_here:(p + 1) * tokens_here]
        at = pl.ds(q * span, span)
        store = pltpu.make_async_copy(out.at[:, at], out_hbm.at[:, at], sem.at[q])
        store.start()
        stores.append(store)
    for store in stores:
        store.wait()


def per_device(nd, ne, tokens, select, gates, w_gate, w_up, w_down):
    tok_dev, width = tokens.shape
    slots = select.shape[1]
    hidden = w_gate.shape[2]
    inner = 2 if nd % 2 == 0 else 1
    outer = nd // inner
    parts = TILE // slots
    batches = 2 if ne % 2 == 0 and (ne // 2 * slots) % 8 == 0 else 1
    each = ne // batches
    rows = each * slots
    stages = 2
    span = width // stages
    wide = span // parts
    fold = max(1, TILE // rows)
    tile_rows = fold * rows
    chunks = width // (fold * wide)
    total_rows = nd * rows
    vmem = pl.BlockSpec(memory_space=pltpu.VMEM)
    hbm = pl.BlockSpec(memory_space=pl.ANY)
    dma = pltpu.SemaphoreType.DMA
    returned, coef = pl.pallas_call(
        functools.partial(kernel, nd, ne),
        out_shape=(
            pltpu.VMEM((stages, ne, TILE, wide), BF16),
            pltpu.VMEM((parts, tok_dev, 3 * ne * TILE), BF16),
        ),
        in_specs=[hbm] * 6,
        out_specs=(vmem, vmem),
        scratch_shapes=[
            pltpu.VMEM((tok_dev, width), BF16),
            pltpu.SMEM(select.shape, jnp.int32),
            pltpu.SMEM(gates.shape, F32),
            pltpu.VMEM((width, hidden), BF16),
            pltpu.VMEM((width, hidden), BF16),
            pltpu.VMEM((hidden, width), BF16),
            pltpu.VMEM((stages, ne, TILE, wide), BF16),
            pltpu.VMEM((batches, stages, inner, outer, each, TILE, wide), BF16),
            pltpu.VMEM((parts * total_rows, parts * total_rows), BF16),
            pltpu.VMEM((total_rows, span), BF16),
            pltpu.VMEM((total_rows, hidden), F32),
            pltpu.VMEM((total_rows, hidden), F32),
            pltpu.VMEM((total_rows, hidden), BF16),
            pltpu.VMEM((batches, chunks, inner, outer, tile_rows, wide), BF16),
            pltpu.VMEM((batches, chunks, outer, tile_rows, wide), BF16),
            pltpu.VMEM((batches, chunks, outer, tile_rows, wide), BF16),
            pltpu.VMEM((batches, chunks, max(outer - 1, 1), tile_rows, wide), BF16),
            pltpu.VMEM((batches, stages, parts * rows, wide), BF16),
            pltpu.VMEM((batches, stages, each, TILE, wide), BF16),
            dma((3,)), dma((3,)),
            dma(()), dma((batches, stages)),
            dma((batches,)), dma((batches, max(outer // 2 - 1, 1))),
            dma((batches, stages, outer)),
            dma(()), dma((batches, stages)),
            dma(()), dma((batches, chunks)),
            dma(()), dma((batches, chunks)),
            dma(()), dma(()),
        ],
        compiler_params=pltpu.CompilerParams(
            collective_id=0, has_side_effects=True, vmem_limit_bytes=60 * 1024 * 1024
        ),
    )(tokens, select, gates, w_gate, w_up, w_down)
    return pl.pallas_call(
        mix,
        out_shape=jax.ShapeDtypeStruct((tok_dev, width), BF16),
        in_specs=[vmem, vmem],
        out_specs=hbm,
        scratch_shapes=[pltpu.VMEM((tok_dev, width), BF16), dma((stages,))],
    )(
        pltpu.with_memory_space_constraint(returned, pltpu.VMEM),
        pltpu.with_memory_space_constraint(coef, pltpu.VMEM),
    )


def solution(mesh):
    return jax.shard_map(
        functools.partial(per_device, mesh.shape["dp"], mesh.shape["expert"]),
        mesh=mesh,
        in_specs=(
            P(("dp", "expert"), None),
            P(None, ("dp", "expert")),
            P(None, ("dp", "expert")),
            P("expert", None, "dp"),
            P("expert", None, "dp"),
            P("expert", "dp", None),
        ),
        out_specs=P(("dp", "expert"), None),
        check_vma=False,
    )
```

```python
import functools

import jax
import jax.numpy as jnp
from jax import lax
from jax.experimental import pallas as pl
from jax.experimental.pallas import tpu as pltpu
from jax.sharding import PartitionSpec as P

MESH = pl.DeviceIdType.MESH
TILE = 16
F32 = jnp.float32
BF16 = jnp.bfloat16
scope = jax.named_scope


def log2(n):
    return n.bit_length() - 1


def kernel(
    nd, ne, tok_hbm, sel_hbm, gat_hbm, wg_hbm, wu_hbm, wd_hbm, ob, cmb, early,
    tok, sel, gat, wg, wu, wd, sb, xp, unp, xs, g_acc, u_acc, hid, pb, xr, zb, zr, summed, rb,
    l_sem, w_sem, a_send, a_recv, gz_send, gf_send, gz_recv, gx_send, gx_recv,
    rx_send, rx_recv, rz_send, rz_recv, o_send, o_recv,
):
    batches, stages, inner, outer, each, _, wide = xp.shape
    slots = sel.shape[1]
    tokens_here = tok.shape[0]
    parts = TILE // slots
    span = wide * parts
    rows = each * slots
    chunks = pb.shape[1]
    tile_rows, tile_cols = pb.shape[4:]
    fold = tile_rows // rows
    cols = fold * tile_cols
    units = ob.shape[0]
    per = chunks // units
    packed = ne * TILE
    total_rows = inner * outer * rows
    half = outer // 2
    pair = 2 if ne % 2 == 0 else 1
    chips = ne // pair
    dp = lax.axis_index("dp")
    ex = lax.axis_index("expert")
    za = dp // inner
    xb = lax.rem(dp, inner)
    other = (inner - 1) - xb
    chip = ex // pair
    core = lax.rem(ex, pair)

    def at_expert(t):
        to_chip = lax.rem(chip + t // pair, chips)
        return to_chip * pair + lax.rem(core + t % pair, pair)

    def at_z(z):
        return (z * inner + xb, ex)

    def at_outer(d):
        return at_z(lax.rem(za + d, outer))

    partner = (za * inner + other, ex)

    def remote(src, dst, send, recv, to):
        return pltpu.make_async_remote_copy(
            src_ref=src, dst_ref=dst, send_sem=send, recv_sem=recv,
            device_id=to, device_id_type=MESH,
        )

    fetch = pltpu.make_async_copy(tok_hbm, tok, l_sem.at[0])
    fetch.start()
    get_sel = pltpu.make_async_copy(sel_hbm, sel, l_sem.at[1])
    get_sel.start()
    get_gat = pltpu.make_async_copy(gat_hbm, gat, l_sem.at[2])
    get_gat.start()
    barrier = pltpu.get_barrier_semaphore()
    for t in range(1, ne):
        pl.semaphore_signal(barrier, inc=1, device_id=(dp, at_expert(t)), device_id_type=MESH)
    for d in range(1, outer):
        pl.semaphore_signal(barrier, inc=1, device_id=at_outer(d), device_id_type=MESH)
    if inner > 1:
        pl.semaphore_signal(barrier, inc=1, device_id=partner, device_id_type=MESH)

    get_sel.wait()
    r_id = lax.broadcasted_iota(jnp.int32, (packed, tokens_here), 0)
    t_id = lax.broadcasted_iota(jnp.int32, (packed, tokens_here), 1)
    r_slot = ((r_id >> log2(TILE)) << log2(slots)) + (r_id & (slots - 1))
    r_part = (r_id & (TILE - 1)) >> log2(slots)
    named = jnp.full((packed, tokens_here), -1, jnp.int32)
    for e in range(ne):
        for s in range(slots):
            named = jnp.where(r_slot == e * slots + s, sel[e, s], named)
    hit = jnp.where(named == t_id, 1.0, 0.0)
    pick = jnp.concatenate(
        [jnp.where(r_part == p, hit, 0.0).astype(BF16) for p in range(parts)], axis=1
    )
    with scope("fetch"):
        fetch.wait()
    loads = [
        pltpu.make_async_copy(h.at[0], v, w_sem.at[i])
        for i, (h, v) in enumerate(((wg_hbm, wg), (wu_hbm, wu), (wd_hbm, wd)))
    ]
    for load in loads:
        load.start()

    def place(e, j):
        r = lax.rem(j - (e // pair) * pair + ne, ne)
        return r // each, lax.rem(r, each)

    mine = place(ex, ex)[1]
    for q in range(stages):
        stack = jnp.concatenate(
            [tok[:, q * span + p * wide:q * span + (p + 1) * wide] for p in range(parts)], axis=0
        )
        gathered = jnp.dot(pick, stack, preferred_element_type=F32).astype(BF16)
        sb[q] = gathered.reshape(ne, TILE, wide)
        xp[0, q, xb, za, mine] = sb[q, ex]

    with scope("barrier"):
        pl.semaphore_wait(barrier, (ne - 1) + (outer - 1) + (1 if inner > 1 else 0))

    for t in range(1, ne):
        for q in range(stages):
            e = at_expert(t)
            b, k = place(e, ex)
            remote(
                sb.at[q, e], xp.at[b, q, xb, za, k], a_send, a_recv.at[b, q], (dp, e)
            ).start()

    relayed = outer >= 4 and outer % 2 == 0 and pair > 1
    my_half = za // max(half, 1)
    near_gate = half - 1 + my_half
    far_gate = half - my_half

    relays = core == pair - 1
    near = sorted(range(1, outer), key=lambda d: min(d, outer - d))

    def mate(i):
        return my_half * half + lax.rem(za - my_half * half + i, half)

    def far_side():
        return [far_gate + i * (1 - 2 * my_half) for i in range(half)]

    def send_own(b, q, k, n):
        block = xp.at[b, q, xb, za, pl.ds(k, n)]
        if inner > 1:
            remote(block, block, gx_send, gx_recv.at[b, q], partner).start()

        def send(z):
            remote(block, block, gz_send.at[b], gz_recv.at[b, q, za], at_z(z)).start()

        if not relayed:
            for d in near:
                send(lax.rem(za + d, outer))
            return
        for i in range(1, half):
            send(mate(i))

        @pl.when(relays)
        def _():
            send(far_gate)

        @pl.when(jnp.logical_not(relays))
        def _():
            for z in far_side():
                send(z)

    def own_first(q):
        send_own(0, q, mine, 1)

    def own(b, q):
        arrived = xp.at[b, q, xb, za, pl.ds(0, each - 1 if b == 0 else each)]
        if b > 0:
            remote(arrived, arrived, a_send, a_recv.at[b, q], partner).wait_recv()
            send_own(b, q, 0, each)
        elif each > 1:
            remote(arrived, arrived, a_send, a_recv.at[b, q], partner).wait_recv()
            for i in range(1, each):
                send_own(b, q, lax.rem(mine + i, each), 1)

    def take(b, q, z):
        block = xp.at[b, q, xb, z]
        remote(block, block, gz_send.at[b], gz_recv.at[b, q, z], partner).wait_recv()
        if inner > 1:
            remote(block, block, gx_send, gx_recv.at[b, q], partner).start()

    def arrive(b, q):
        if not relayed:
            for d in near:
                take(b, q, lax.rem(za + outer - d, outer))
            return
        for i in range(1, half):
            take(b, q, mate(i))

    def relay(b, q):
        if not relayed:
            return

        @pl.when(relays & (za == near_gate))
        def _():
            for z in far_side():
                take(b, q, z)
                block = xp.at[b, q, xb, z]
                for i in range(1, half):
                    remote(
                        block, block, gf_send.at[b, i - 1], gz_recv.at[b, q, z], at_z(mate(i))
                    ).start()

    def distant(b, q):
        if not relayed:
            return

        @pl.when(jnp.logical_not(relays & (za == near_gate)))
        def _():
            for z in far_side():
                take(b, q, z)

    def spread():
        r = lax.broadcasted_iota(jnp.int32, unp.shape, 0)
        k = lax.broadcasted_iota(jnp.int32, unp.shape, 1)
        part = r >> log2(total_rows)
        row = r & (total_rows - 1)
        col = ((row >> log2(slots)) << log2(TILE)) + (part << log2(slots)) + (row & (slots - 1))
        unp[...] = jnp.where(k == col, 1.0, 0.0).astype(BF16)

    step = min(256, hid.shape[1])
    blocks = hid.shape[1] // step

    def ready(b, q):
        if inner > 1:
            block = xp.at[b, q, other]
            remote(block, block, gx_send, gx_recv.at[b, q], partner).wait_recv()
        if b == 0 and q == 0:
            loads[0].wait()
            loads[1].wait()
        flat = jnp.dot(
            unp[...], xp[b, q].reshape(parts * total_rows, wide), preferred_element_type=F32
        ).astype(BF16)
        for p in range(parts):
            xs[:, p * wide:(p + 1) * wide] = flat[p * total_rows:(p + 1) * total_rows]

    def multiply(b, q, i):
        at = pl.ds(i * step, step)
        g = jnp.dot(xs[...], wg[q * span:(q + 1) * span, at], preferred_element_type=F32)
        u = jnp.dot(xs[...], wu[q * span:(q + 1) * span, at], preferred_element_type=F32)
        if q > 0:
            g = g + g_acc[:, at]
            u = u + u_acc[:, at]
        if q < stages - 1:
            g_acc[:, at] = g
            u_acc[:, at] = u
        else:
            hid[:, at] = (g / (1.0 + jnp.exp(-g)) * u).astype(BF16)

    def rx(b, c):
        return remote(pb.at[b, c, other], xr.at[b, c], rx_send, rx_recv.at[b, c], partner)

    def down(b, c):
        if b == 0 and c == 0:
            loads[2].wait()
        at = pl.ds(c * cols, cols)
        part = jnp.dot(hid[...], wd[:, at], preferred_element_type=F32)
        part = part.reshape(inner, outer, rows, cols)
        part = jnp.concatenate(
            [part[..., f * tile_cols:(f + 1) * tile_cols] for f in range(fold)], axis=2
        )
        pb[b, c] = part.astype(BF16)
        if inner > 1:
            rx(b, c).start()

    def inner_sum(b, c):
        value = pb[b, c, xb].astype(F32)
        if inner > 1:
            rx(b, c).wait_recv()
            value = value + xr[b, c].astype(F32)
        zb[b, c] = value.astype(BF16)
        if relayed:
            order_z = far_side()[::-1] + [mate(i) for i in range(1, half)]
        else:
            order_z = [lax.rem(za + d, outer) for d in near[::-1]]
        for to in order_z:
            slot = lax.rem(to - za + outer, outer) - 1
            remote(
                zb.at[b, c, to], zr.at[b, c, slot], rz_send, rz_recv.at[b, c], at_z(to)
            ).start()

    def packing():
        r = lax.broadcasted_iota(jnp.int32, (each * TILE, parts * rows), 0)
        k = lax.broadcasted_iota(jnp.int32, (each * TILE, parts * rows), 1)
        col = (
            ((r & (TILE - 1)) >> log2(slots)) * rows
            + ((r >> log2(TILE)) << log2(slots)) + (r & (slots - 1))
        )
        return jnp.where(k == col, 1.0, 0.0).astype(BF16)

    def outer_sum(b, c):
        value = zb[b, c, za].astype(F32)
        if outer > 1:
            remote(zr.at[b, c], zr.at[b, c], rz_send, rz_recv.at[b, c], partner).wait_recv()
            for d in range(1, outer):
                value = value + zr[b, c, d - 1].astype(F32)
        unit, i = c // per, c % per
        summed[b, unit, i * tile_rows:(i + 1) * tile_rows] = value.astype(BF16)
        if i == per - 1:
            give(b, unit)

    def give(b, unit):
        back = jnp.dot(packing(), summed[b, unit], preferred_element_type=F32)
        rb[b, unit] = back.astype(BF16).reshape(each, TILE, wide)
        if b == 0:
            ob[unit, ex] = rb[b, unit, mine]
            ks = [lax.rem(mine + i, each) for i in range(1, each)]
        else:
            ks = list(range(each))
        for k in ks:
            j = lax.rem(chip * pair + b * each + k, ne)
            remote(rb.at[b, unit, k], ob.at[unit, ex], o_send, o_recv.at[unit], (dp, j)).start()

    def weigh():
        get_gat.wait()
        terms = 3
        c_id = lax.broadcasted_iota(jnp.int32, (tokens_here, terms * packed), 1)
        n_id = lax.broadcasted_iota(jnp.int32, (tokens_here, terms * packed), 0)
        c_row = c_id & (packed - 1)
        c_slot = ((c_row >> log2(TILE)) << log2(slots)) + (c_row & (slots - 1))
        weight = jnp.zeros((tokens_here, terms * packed), F32)
        for e in range(ne):
            for s in range(slots):
                weight = jnp.where(
                    (c_slot == e * slots + s) & (n_id == sel[e, s]), gat[e, s], weight
                )
        left = weight
        coef = jnp.zeros_like(weight)
        for i in range(terms):
            term = left.astype(BF16).astype(F32)
            coef = jnp.where((c_id >> log2(packed)) == i, term, coef)
            left = left - term
        c_part = (c_row & (TILE - 1)) >> log2(slots)
        for p in range(parts):
            cmb[p] = jnp.where(c_part == p, coef, 0.0).astype(BF16)

    tasks = dict(
        first=own_first, own=own, arrive=arrive, relay=relay, distant=distant, spread=spread, ready=ready, mult=multiply,
        down=down, inner=inner_sum, outer=outer_sum, weigh=weigh,
    )
    for name, *args in order(batches, stages, blocks, chunks):
        with scope("_".join([name] + [str(a) for a in args])):
            tasks[name](*args)

    def drain(block, sem):
        remote(block, block, sem, sem, partner).wait_send()

    for unit in range(units):
        with scope("back"):
            landed = ob.at[unit, 0:ne - 1]
            remote(landed, landed, o_send, o_recv.at[unit], partner).wait_recv()
        if unit < units - 1:
            blend(ob, cmb, unit, early, unit * span)
    landed = ob.at[:, 0:ne - 1]
    drain(sb.at[:, 0:ne - 1], a_send)
    drain(landed, o_send)
    if outer > 1:
        drain(zb.at[:, :, 0:outer - 1], rz_send)
        if not relayed:
            for b in range(batches):
                drain(xp.at[b, :, 0, 0:outer - 1], gz_send.at[b])
        else:
            @pl.when(relays)
            def _():
                for b in range(batches):
                    drain(xp.at[b, :, 0, 0:half], gz_send.at[b])

            @pl.when(jnp.logical_not(relays))
            def _():
                for b in range(batches):
                    drain(xp.at[b, :, 0, 0:outer - 1], gz_send.at[b])

            @pl.when(relays & (za == near_gate))
            def _():
                for b in range(batches):
                    for i in range(half - 1):
                        drain(xp.at[b, :, 0, 0:half], gf_send.at[b, i])
    if inner > 1:
        drain(xp.at[:, :, 0], gx_send)
        drain(pb.at[:, :, 0], rx_send)


def order(batches, stages, blocks, chunks):
    last = batches - 1
    both = range(batches)
    for q in range(stages):
        yield ("first", q)
        yield ("own", 0, q)
    yield ("spread",)
    if last:
        yield from (("own", 1, q) for q in range(stages))
    for q in range(stages):
        yield ("arrive", 0, q)
        yield ("relay", 0, q)
    yield from (("distant", 0, q) for q in range(stages))
    if last:
        yield from (("arrive", 1, q) for q in range(stages))
    yield ("weigh",)
    for q in range(stages):
        if last:
            yield ("relay", 1, q)
        yield ("ready", 0, q)
        for i in range(blocks):
            yield ("mult", 0, q, i)
        if last:
            yield ("distant", 1, q)
    n = 0
    if last:
        yield ("down", 0, 0)
        yield ("down", 0, 1)
        for q in range(stages):
            yield ("ready", 1, q)
            for i in range(blocks):
                yield ("mult", 1, q, i)
                if q == 0 and i % 2 == 1:
                    yield ("down", 0, 2 + i // 2)
                if q > 0 and i % 2 == 1 and n < chunks:
                    yield ("inner", 0, n)
                    n += 1
        for c in range(chunks):
            yield ("down", 1, c)
            if c % 2 == 1 and n < chunks:
                yield ("inner", 0, n)
                n += 1
    for c in range(n, chunks):
        yield ("inner", 0, c)
    lag = 1
    for c in range(chunks + lag):
        if last and c < chunks:
            yield ("inner", 1, c)
        if c >= lag:
            yield ("outer", 0, c - lag)
    if last:
        yield from (("outer", 1, c) for c in range(chunks))


def blend(ob, cmb, unit, out, start):
    _, ne, tile, wide = ob.shape
    parts, tokens_here, depth = cmb.shape
    packed = ne * tile
    got = ob[unit].reshape(packed, wide)
    total = jnp.dot(
        cmb[...].reshape(parts * tokens_here, depth),
        jnp.concatenate([got] * (depth // packed), axis=0),
        preferred_element_type=F32,
    ).astype(BF16)
    for p in range(parts):
        at = start + p * wide
        out[:, at:at + wide] = total[p * tokens_here:(p + 1) * tokens_here]


def mix(ob, cmb, early, out_hbm, late, sem):
    done = early.shape[1]
    first = pltpu.make_async_copy(early, out_hbm.at[:, pl.ds(0, done)], sem.at[0])
    first.start()
    blend(ob, cmb, ob.shape[0] - 1, late, 0)
    second = pltpu.make_async_copy(late, out_hbm.at[:, pl.ds(done, late.shape[1])], sem.at[1])
    second.start()
    first.wait()
    second.wait()


def per_device(nd, ne, tokens, select, gates, w_gate, w_up, w_down):
    tok_dev, width = tokens.shape
    slots = select.shape[1]
    hidden = w_gate.shape[2]
    inner = 2 if nd % 2 == 0 else 1
    outer = nd // inner
    parts = TILE // slots
    batches = 2 if ne % 2 == 0 and (ne // 2 * slots) % 8 == 0 else 1
    each = ne // batches
    rows = each * slots
    stages = 2
    span = width // stages
    wide = span // parts
    fold = max(1, TILE // rows)
    tile_rows = fold * rows
    chunks = width // (fold * wide)
    total_rows = nd * rows
    vmem = pl.BlockSpec(memory_space=pltpu.VMEM)
    hbm = pl.BlockSpec(memory_space=pl.ANY)
    dma = pltpu.SemaphoreType.DMA
    handed = pl.pallas_call(
        functools.partial(kernel, nd, ne),
        out_shape=(
            pltpu.VMEM((stages, ne, TILE, wide), BF16),
            pltpu.VMEM((parts, tok_dev, 3 * ne * TILE), BF16),
            pltpu.VMEM((tok_dev, width - span), BF16),
        ),
        in_specs=[hbm] * 6,
        out_specs=(vmem, vmem, vmem),
        scratch_shapes=[
            pltpu.VMEM((tok_dev, width), BF16),
            pltpu.SMEM(select.shape, jnp.int32),
            pltpu.SMEM(gates.shape, F32),
            pltpu.VMEM((width, hidden), BF16),
            pltpu.VMEM((width, hidden), BF16),
            pltpu.VMEM((hidden, width), BF16),
            pltpu.VMEM((stages, ne, TILE, wide), BF16),
            pltpu.VMEM((batches, stages, inner, outer, each, TILE, wide), BF16),
            pltpu.VMEM((parts * total_rows, parts * total_rows), BF16),
            pltpu.VMEM((total_rows, span), BF16),
            pltpu.VMEM((total_rows, hidden), F32),
            pltpu.VMEM((total_rows, hidden), F32),
            pltpu.VMEM((total_rows, hidden), BF16),
            pltpu.VMEM((batches, chunks, inner, outer, tile_rows, wide), BF16),
            pltpu.VMEM((batches, chunks, outer, tile_rows, wide), BF16),
            pltpu.VMEM((batches, chunks, outer, tile_rows, wide), BF16),
            pltpu.VMEM((batches, chunks, max(outer - 1, 1), tile_rows, wide), BF16),
            pltpu.VMEM((batches, stages, parts * rows, wide), BF16),
            pltpu.VMEM((batches, stages, each, TILE, wide), BF16),
            dma((3,)), dma((3,)),
            dma(()), dma((batches, stages)),
            dma((batches,)), dma((batches, max(outer // 2 - 1, 1))),
            dma((batches, stages, outer)),
            dma(()), dma((batches, stages)),
            dma(()), dma((batches, chunks)),
            dma(()), dma((batches, chunks)),
            dma(()), dma((stages,)),
        ],
        compiler_params=pltpu.CompilerParams(
            collective_id=0, has_side_effects=True, vmem_limit_bytes=60 * 1024 * 1024
        ),
    )(tokens, select, gates, w_gate, w_up, w_down)
    return pl.pallas_call(
        mix,
        out_shape=jax.ShapeDtypeStruct((tok_dev, width), BF16),
        in_specs=[vmem] * 3,
        out_specs=hbm,
        scratch_shapes=[pltpu.VMEM((tok_dev, span), BF16), dma((2,))],
    )(*[pltpu.with_memory_space_constraint(array, pltpu.VMEM) for array in handed])


def solution(mesh):
    return jax.shard_map(
        functools.partial(per_device, mesh.shape["dp"], mesh.shape["expert"]),
        mesh=mesh,
        in_specs=(
            P(("dp", "expert"), None),
            P(None, ("dp", "expert")),
            P(None, ("dp", "expert")),
            P("expert", None, "dp"),
            P("expert", None, "dp"),
            P("expert", "dp", None),
        ),
        out_specs=P(("dp", "expert"), None),
        check_vma=False,
    )
```
